512 devices in a mesh: frag: 64 (over y, z_hi, core), band: 8 (over x, z_lo).
Axes of the slice: x: 4, y: 8, z: 8 (z_hi: 4, z_lo: 2; z = z_hi * 2 + z_lo), core: 2. Of those that a mesh axis runs over, the one named last changes fastest.
Arguments:
- orbitals: bfloat16 [16384, 32768], P(('frag', 'band')), parts along dimension 0, may hold values from -40 to 40
- potential: float32 [2097152], P('frag'), parts along dimension 0, may hold values from 0.5 to 3
Outputs:
- margin: float32 [16384, 256], P(('frag', 'band')), parts along dimension 0
- projected: float32 [16384, 256], P(('frag', 'band')), parts along dimension 0
- residuals: bfloat16 [16384, 32768], P(('frag', 'band')), parts along dimension 0
The draws below stay inside these ranges and needn't reach their ends.
There are 64 independent parts, one for each index of `frag`. The reference program is written for one: setup_inputs(seed, part) draws one part's arguments, and reference() takes and returns one part's arrays. A program takes and returns all parts, laid end to end along the dimension named above; each array names one. Nothing has to cross between parts.
All inputs are finite; a program needn't handle non-finite values.
Results may differ from the reference program's by a relative error of at most 0.034.
Values may be sent and summed in bfloat16 or wider, within the bound.
A program may use at most 128 MiB of HBM per device.

```python
import math
import jax
import jax.numpy as jnp

NSIDE = 32
BANDS = 256
GRID = 32768


def draw_orbitals(key, part):
    key_scale = jax.random.fold_in(key, 11)
    key_base = jax.random.fold_in(key, 12)
    scales = jnp.exp(jax.random.uniform(key_scale, (BANDS, 1), jnp.float32, math.log(0.5), math.log(5.0)))
    base = jnp.clip(jax.random.normal(key_base, (BANDS, GRID), jnp.float32), -6.0, 6.0)
    return (base * scales).astype(jnp.bfloat16)


def setup_inputs(seed: int = 0, part: int = 0) -> dict:
    key_list = jax.random.split(jax.random.key(seed), 3)
    part_splits = jax.random.split(jax.random.fold_in(key_list[2], part), 3)
    orbitals = draw_orbitals(jax.random.fold_in(jax.random.fold_in(key_list[2], part), 71), part)
    potential = jnp.clip(jax.random.uniform(part_splits[1], (GRID,), jnp.float32, 0.5, 3.0), 0.5, 3.0)
    return dict(orbitals=orbitals, potential=potential)


def apply_hamiltonian(orbitals, potential):
    field = orbitals.astype(jnp.float32).reshape(BANDS, NSIDE, NSIDE, NSIDE)
    beside_all = jnp.zeros_like(field)
    for axis in (1, 2, 3):
        beside_all = beside_all + jnp.roll(field, 1, axis) + jnp.roll(field, -1, axis)
    pot = potential.reshape(1, NSIDE, NSIDE, NSIDE)
    result = 0.5 * (6.0 * field - beside_all) + pot * field
    return result.reshape(BANDS, GRID).astype(jnp.bfloat16)


def reference(orbitals, potential):
    applied = apply_hamiltonian(orbitals, potential)
    margin = jnp.dot(orbitals, orbitals.T, preferred_element_type=jnp.float32)
    projected = jnp.dot(applied, orbitals.T, preferred_element_type=jnp.float32)
    coefficients = (projected / jnp.diagonal(margin)[:, None]).astype(jnp.bfloat16)
    mixed = jnp.dot(coefficients, orbitals, preferred_element_type=jnp.float32)
    residuals = (applied.astype(jnp.float32) - mixed).astype(jnp.bfloat16)
    return margin, projected, residuals
```

```python
import functools

import jax
import jax.numpy as jnp
from jax import lax
from jax.experimental import pallas as pl
from jax.experimental.pallas import tpu as pltpu
from jax.sharding import PartitionSpec as P

MESH = pl.DeviceIdType.MESH
SIDE = 32
PLANE = SIDE * SIDE
LANES = 128
SLICES = PLANE // LANES
OWN = 32
BANDS = 256
PEERS = 8
DEPTH = SIDE // PEERS
OFFSETS = ((2, 1), (2, 0), (1, 1), (3, 1), (1, 0), (3, 0), (0, 1))
FIRST = 0
GATE_AT = 3


def contract_rows(left, right):
    return lax.dot_general(left, right, (((1,), (1,)), ((), ())), preferred_element_type=jnp.float32)


def kernel(
    phi_hbm, pot_hbm, out_ref, margin_ref, projected_ref,
    phi, pot, applied, block, half, margin_sum, half_sum,
    margin_send, margin_recv, proj_send, proj_recv, coef_send, coef, mixed, back,
    load_sem, phi_ss, phi_rs, margin_ss, margin_rs, proj_ss, proj_rs, coef_ss, coef_rs, back_ss, back_rs, gate,
):
    me = lax.axis_index("band")
    frag = lax.axis_index("frag")
    core = lax.rem(frag, 2)
    x, z = me // 2, lax.rem(me, 2)
    partner = frag + 1 - 2 * core

    def peer(j):
        dx, dz = OFFSETS[j]
        return lax.rem(x + dx, 4) * 2 + lax.rem(z + dz, 2)

    def source(j):
        dx, dz = OFFSETS[j]
        return lax.rem(x + 4 - dx, 4) * 2 + lax.rem(z + dz, 2)

    def rows(b):
        return pl.ds(pl.multiple_of(b * OWN, OWN), OWN)

    def cols(plane, c=0, n=PLANE):
        return pl.ds(pl.multiple_of(plane * PLANE + c * LANES, LANES), n)

    barrier = pltpu.get_barrier_semaphore()
    for j in range(PEERS - 1):
        pl.semaphore_signal(barrier, inc=1, device_id={"band": peer(j)}, device_id_type=MESH)
    pl.semaphore_signal(barrier, inc=1, device_id={"frag": partner}, device_id_type=MESH)
    loads = [pltpu.make_async_copy(pot_hbm, pot, load_sem.at[4])]
    for i in range(4):
        part = pl.ds(i * 8 * PLANE, 8 * PLANE)
        loads.append(pltpu.make_async_copy(phi_hbm.at[:, part], phi.at[:, part], load_sem.at[i]))
    for load in loads:
        load.start()
    for load in loads:
        load.wait()
    pl.semaphore_wait(barrier, PEERS)

    lane = lax.broadcasted_iota(jnp.int32, (OWN, LANES), 1)
    z_pos = lax.rem(lane, SIDE)
    z_last, z_first = z_pos == SIDE - 1, z_pos == 0
    y_inner, y_outer = lane < LANES - SIDE, lane >= SIDE

    def upper(fields):
        ahead = [pltpu.roll(f, LANES - SIDE, 1) for f in fields]
        sums = []
        for c in range(SLICES):
            y_up = jnp.where(y_inner, ahead[c], ahead[(c + 1) % SLICES])
            z_up = jnp.where(z_last, pltpu.roll(fields[c], SIDE - 1, 1), pltpu.roll(fields[c], LANES - 1, 1))
            sums.append(y_up + z_up)
        return sums

    def lower(fields):
        behind = [pltpu.roll(f, SIDE, 1) for f in fields]
        sums = []
        for c in range(SLICES):
            y_down = jnp.where(y_outer, behind[c], behind[(c - 1) % SLICES])
            z_down = jnp.where(z_first, pltpu.roll(fields[c], LANES - SIDE + 1, 1), pltpu.roll(fields[c], 1, 1))
            sums.append(y_down + z_down)
        return sums

    def phi_copy(j, k):
        plane = lax.rem(peer(j) * DEPTH + k, SIDE)
        return pltpu.make_async_remote_copy(
            src_ref=phi.at[:, cols(plane)], dst_ref=block.at[k, rows(me), :],
            send_sem=phi_ss.at[k, j], recv_sem=phi_rs.at[k, j],
            device_id={"band": peer(j)}, device_id_type=MESH)

    def phi_arrival(j, k):
        return pltpu.make_async_remote_copy(
            src_ref=phi.at[:, cols(0)], dst_ref=block.at[k, rows(source(j)), :],
            send_sem=phi_ss.at[k, j], recv_sem=phi_rs.at[k, j],
            device_id={"band": peer(j)}, device_id_type=MESH)

    def back_copy(j, k):
        return pltpu.make_async_remote_copy(
            src_ref=mixed.at[k, rows(peer(j)), :], dst_ref=back.at[k, me],
            send_sem=back_ss.at[k, j], recv_sem=back_rs.at[k, j],
            device_id={"band": peer(j)}, device_id_type=MESH)

    def back_arrival(j, k):
        return pltpu.make_async_remote_copy(
            src_ref=mixed.at[k, rows(peer(j)), :], dst_ref=back.at[k, source(j)],
            send_sem=back_ss.at[k, j], recv_sem=back_rs.at[k, j],
            device_id={"band": peer(j)}, device_id_type=MESH)

    def terms_copy(j, sent, received, ss, rs):
        return pltpu.make_async_remote_copy(
            src_ref=sent.at[rows(peer(j)), :], dst_ref=received.at[j],
            send_sem=ss.at[j], recv_sem=rs.at[j],
            device_id={"band": peer(j)}, device_id_type=MESH)

    def coef_copy(j):
        return pltpu.make_async_remote_copy(
            src_ref=coef_send, dst_ref=coef.at[rows(me), :],
            send_sem=coef_ss.at[j], recv_sem=coef_rs.at[j],
            device_id={"band": peer(j)}, device_id_type=MESH)

    def coef_arrival(j):
        return pltpu.make_async_remote_copy(
            src_ref=coef_send, dst_ref=coef.at[rows(source(j)), :],
            send_sem=coef_ss.at[j], recv_sem=coef_rs.at[j],
            device_id={"band": peer(j)}, device_id_type=MESH)

    def send_phi():
        def planes(k, carry):
            for j in range(PEERS - 1):
                phi_copy(j, k).start()
            return carry
        lax.fori_loop(0, DEPTH + 1, planes, 0)

    @pl.when(core == FIRST)
    def _():
        send_phi()

    def own_block(k, carry):
        plane = lax.rem(me * DEPTH + k, SIDE)
        block[k, rows(me), :] = phi[:, cols(plane)]
        return carry
    lax.fori_loop(0, DEPTH + 1, own_block, 0)

    def apply_plane(g, carry):
        fields = [phi[:, cols(g, c, LANES)].astype(jnp.float32) for c in range(SLICES)]
        ups, downs = upper(fields), lower(fields)
        after, before = lax.rem(g + 1, SIDE), lax.rem(g + SIDE - 1, SIDE)
        for c in range(SLICES):
            beside = ups[c] + downs[c]
            beside += phi[:, cols(after, c, LANES)].astype(jnp.float32)
            beside += phi[:, cols(before, c, LANES)].astype(jnp.float32)
            weight = pot[pl.ds(g * SLICES + c, 1), :] + 3.0
            applied[:, cols(g, c, LANES)] = (weight * fields[c] - 0.5 * beside).astype(jnp.bfloat16)
        return carry
    lax.fori_loop(0, SIDE, apply_plane, 0)

    @pl.when(core != FIRST)
    def _():
        pl.semaphore_wait(gate, 1)
        send_phi()

    def half_stencil(k, with_next):
        def some_rows(i, carry):
            r = rows(i)
            fields = [block[k, r, c * LANES:(c + 1) * LANES].astype(jnp.float32) for c in range(SLICES)]
            ups = upper(fields)
            for c in range(SLICES):
                beside = ups[c]
                if with_next:
                    beside += block[k + 1, r, c * LANES:(c + 1) * LANES].astype(jnp.float32)
                weight = 0.5 * pot[pl.ds((me * DEPTH + k) * SLICES + c, 1), :] + 1.5
                half[r, c * LANES:(c + 1) * LANES] = (weight * fields[c] - 0.5 * beside).astype(jnp.bfloat16)
            return carry
        lax.fori_loop(0, PEERS, some_rows, 0)

    for k in range(DEPTH):
        for j in range(PEERS - 1):
            phi_arrival(j, k).wait_recv()
        if k == GATE_AT:
            @pl.when(core == FIRST)
            def _():
                pl.semaphore_signal(gate, inc=1, device_id={"frag": partner}, device_id_type=MESH)
        term = contract_rows(block[k], block[k])
        margin_sum[...] = term if k == 0 else margin_sum[...] + term
        if k == DEPTH - 1:
            margin_send[...] = margin_sum[...].astype(jnp.bfloat16)
            for j in range(PEERS - 1):
                terms_copy(j, margin_send, margin_recv, margin_ss, margin_rs).start()
        if k >= 1:
            half_stencil(k - 1, True)
            term = contract_rows(block[k - 1], half[...])
            half_sum[...] = term if k == 1 else half_sum[...] + term
    half_stencil(DEPTH - 1, False)
    half_sum[...] += contract_rows(block[DEPTH - 1], half[...])
    for j in range(PEERS - 1):
        phi_arrival(j, DEPTH).wait_recv()
    total = half_sum[...] - 0.5 * contract_rows(block[DEPTH - 1], block[DEPTH])
    total = total + total.T
    half_sum[...] = total
    proj_send[...] = total.astype(jnp.bfloat16)
    for j in range(PEERS - 1):
        terms_copy(j, proj_send, proj_recv, proj_ss, proj_rs).start()

    column = lax.broadcasted_iota(jnp.int32, (OWN, BANDS), 1)
    row = lax.broadcasted_iota(jnp.int32, (OWN, BANDS), 0)
    on_diagonal = column == row + me * OWN
    margin = margin_sum[rows(me), :]
    for j in range(PEERS - 1):
        terms_copy(j, margin_send, margin_recv, margin_ss, margin_rs).wait_recv()
        margin += margin_recv[j].astype(jnp.float32)
    margin_ref[...] = margin
    diagonal = jnp.sum(jnp.where(on_diagonal, margin, 0.0), axis=1, keepdims=True)
    projected = half_sum[rows(me), :]
    for j in range(PEERS - 1):
        terms_copy(j, proj_send, proj_recv, proj_ss, proj_rs).wait_recv()
        projected += proj_recv[j].astype(jnp.float32)
    projected_ref[...] = projected
    rounded = (projected / diagonal).astype(jnp.bfloat16).astype(jnp.float32)
    own_coef = jnp.sum(jnp.where(on_diagonal, rounded, 0.0), axis=1, keepdims=True)
    others = jnp.where(on_diagonal, 0.0, rounded).astype(jnp.bfloat16)
    coef_send[...] = others
    for j in range(PEERS - 1):
        coef_copy(j).start()
    coef[rows(me), :] = others
    for j in range(PEERS - 1):
        coef_arrival(j).wait_recv()

    for k in range(DEPTH):
        mixed[k] = jnp.dot(coef[...], block[k], preferred_element_type=jnp.float32).astype(jnp.bfloat16)
        for j in range(PEERS - 1):
            back_copy(j, k).start()

    def finish(k, b, taken):
        plane = b * DEPTH + k
        for c in range(SLICES):
            rest = applied[:, cols(plane, c, LANES)].astype(jnp.float32)
            rest -= own_coef * phi[:, cols(plane, c, LANES)].astype(jnp.float32)
            out_ref[:, cols(plane, c, LANES)] = (rest - taken(c).astype(jnp.float32)).astype(jnp.bfloat16)

    def finish_own(k, carry):
        finish(k, me, lambda c: mixed[k, rows(me), c * LANES:(c + 1) * LANES])
        return carry
    lax.fori_loop(0, DEPTH, finish_own, 0)

    def finish_others(k, carry):
        for j in range(PEERS - 1):
            back_arrival(j, k).wait_recv()
            b = source(j)
            finish(k, b, lambda c: back[k, b, :, c * LANES:(c + 1) * LANES])
        return carry
    lax.fori_loop(0, DEPTH, finish_others, 0)

    for j in range(PEERS - 1):
        terms_copy(j, margin_send, margin_recv, margin_ss, margin_rs).wait_send()
        terms_copy(j, proj_send, proj_recv, proj_ss, proj_rs).wait_send()
        coef_copy(j).wait_send()

    def drain_phi(k, carry):
        for j in range(PEERS - 1):
            phi_copy(j, k).wait_send()
        return carry
    lax.fori_loop(0, DEPTH + 1, drain_phi, 0)

    def drain_back(k, carry):
        for j in range(PEERS - 1):
            back_copy(j, k).wait_send()
        return carry
    lax.fori_loop(0, DEPTH, drain_back, 0)


def shards(orbitals, potential):
    grid = orbitals.shape[1]
    bf16, f32 = jnp.bfloat16, jnp.float32
    dma = pltpu.SemaphoreType.DMA
    residuals, margin, projected = pl.pallas_call(
        kernel,
        out_shape=(
            jax.ShapeDtypeStruct((OWN, grid), bf16),
            jax.ShapeDtypeStruct((OWN, BANDS), f32),
            jax.ShapeDtypeStruct((OWN, BANDS), f32),
        ),
        in_specs=[pl.BlockSpec(memory_space=pl.ANY)] * 2,
        out_specs=[pl.BlockSpec(memory_space=pltpu.VMEM)] * 3,
        scratch_shapes=[
            pltpu.VMEM((OWN, grid), bf16),
            pltpu.VMEM((grid // LANES, LANES), f32),
            pltpu.VMEM((OWN, grid), bf16),
            pltpu.VMEM((DEPTH + 1, BANDS, PLANE), bf16),
            pltpu.VMEM((BANDS, PLANE), bf16),
            pltpu.VMEM((BANDS, BANDS), f32),
            pltpu.VMEM((BANDS, BANDS), f32),
            pltpu.VMEM((BANDS, BANDS), bf16),
            pltpu.VMEM((PEERS - 1, OWN, BANDS), bf16),
            pltpu.VMEM((BANDS, BANDS), bf16),
            pltpu.VMEM((PEERS - 1, OWN, BANDS), bf16),
            pltpu.VMEM((OWN, BANDS), bf16),
            pltpu.VMEM((BANDS, BANDS), bf16),
            pltpu.VMEM((DEPTH, BANDS, PLANE), bf16),
            pltpu.VMEM((DEPTH, PEERS, OWN, PLANE), bf16),
            dma((5,)),
            dma((DEPTH + 1, PEERS - 1)),
            dma((DEPTH + 1, PEERS - 1)),
            dma((PEERS - 1,)),
            dma((PEERS - 1,)),
            dma((PEERS - 1,)),
            dma((PEERS - 1,)),
            dma((PEERS - 1,)),
            dma((PEERS - 1,)),
            dma((DEPTH, PEERS - 1)),
            dma((DEPTH, PEERS - 1)),
            pltpu.SemaphoreType.REGULAR,
        ],
        compiler_params=pltpu.CompilerParams(collective_id=0, has_side_effects=True),
        name="subspace",
    )(orbitals, potential.reshape(grid // LANES, LANES))
    return margin, projected, residuals


def solution(mesh):
    return jax.shard_map(
        shards,
        mesh=mesh,
        in_specs=(P(("frag", "band"), None), P("frag")),
        out_specs=(P(("frag", "band"), None), P(("frag", "band"), None), P(("frag", "band"), None)),
        check_vma=False,
    )
```

```python
import functools

import jax
import jax.numpy as jnp
from jax import lax
from jax.experimental import pallas as pl
from jax.experimental.pallas import tpu as pltpu
from jax.sharding import PartitionSpec as P

MESH = pl.DeviceIdType.MESH
SIDE = 32
PLANE = SIDE * SIDE
LANES = 128
SLICES = PLANE // LANES
OWN = 32
BANDS = 256
PEERS = 8
DEPTH = SIDE // PEERS
OFFSETS = ((2, 1), (2, 0), (1, 1), (3, 1), (1, 0), (3, 0), (0, 1))
FIRST = 1
GATE_AT = 2
GATE_BACK_AT = 3


def contract_rows(left, right):
    return lax.dot_general(left, right, (((1,), (1,)), ((), ())), preferred_element_type=jnp.float32)


def kernel(
    phi_hbm, pot_hbm, out_ref, margin_ref, projected_ref,
    phi, pot, applied, block, half, margin_sum, half_sum,
    terms_send, terms_recv, coef_send, coef, mixed, back,
    load_sem, phi_ss, phi_rs, terms_ss, terms_rs, coef_ss, coef_rs, back_ss, back_rs, gate, gate_back,
):
    me = lax.axis_index("band")
    frag = lax.axis_index("frag")
    core = lax.rem(frag, 2)
    x, z = me // 2, lax.rem(me, 2)
    partner = frag + 1 - 2 * core

    def peer(j):
        dx, dz = OFFSETS[j]
        return lax.rem(x + dx, 4) * 2 + lax.rem(z + dz, 2)

    def source(j):
        dx, dz = OFFSETS[j]
        return lax.rem(x + 4 - dx, 4) * 2 + lax.rem(z + dz, 2)

    def rows(b):
        return pl.ds(pl.multiple_of(b * OWN, OWN), OWN)

    def cols(plane, c=0, n=PLANE):
        return pl.ds(pl.multiple_of(plane * PLANE + c * LANES, LANES), n)

    barrier = pltpu.get_barrier_semaphore()
    for j in range(PEERS - 1):
        pl.semaphore_signal(barrier, inc=1, device_id={"band": peer(j)}, device_id_type=MESH)
    pl.semaphore_signal(barrier, inc=1, device_id={"frag": partner}, device_id_type=MESH)
    loads = [pltpu.make_async_copy(pot_hbm, pot, load_sem.at[4])]
    for i in range(4):
        part = pl.ds(i * 8 * PLANE, 8 * PLANE)
        loads.append(pltpu.make_async_copy(phi_hbm.at[:, part], phi.at[:, part], load_sem.at[i]))
    for load in loads:
        load.start()
    for load in loads:
        load.wait()
    pl.semaphore_wait(barrier, PEERS)

    lane = lax.broadcasted_iota(jnp.int32, (OWN, LANES), 1)
    z_pos = lax.rem(lane, SIDE)
    z_last, z_first = z_pos == SIDE - 1, z_pos == 0
    y_inner, y_outer = lane < LANES - SIDE, lane >= SIDE

    def upper(fields):
        ahead = [pltpu.roll(f, LANES - SIDE, 1) for f in fields]
        sums = []
        for c in range(SLICES):
            y_up = jnp.where(y_inner, ahead[c], ahead[(c + 1) % SLICES])
            z_up = jnp.where(z_last, pltpu.roll(fields[c], SIDE - 1, 1), pltpu.roll(fields[c], LANES - 1, 1))
            sums.append(y_up + z_up)
        return sums

    def lower(fields):
        behind = [pltpu.roll(f, SIDE, 1) for f in fields]
        sums = []
        for c in range(SLICES):
            y_down = jnp.where(y_outer, behind[c], behind[(c - 1) % SLICES])
            z_down = jnp.where(z_first, pltpu.roll(fields[c], LANES - SIDE + 1, 1), pltpu.roll(fields[c], 1, 1))
            sums.append(y_down + z_down)
        return sums

    def phi_copy(j, k):
        plane = lax.rem(peer(j) * DEPTH + k, SIDE)
        return pltpu.make_async_remote_copy(
            src_ref=phi.at[:, cols(plane)], dst_ref=block.at[k, rows(me), :],
            send_sem=phi_ss.at[k, j], recv_sem=phi_rs.at[k, j],
            device_id={"band": peer(j)}, device_id_type=MESH)

    def phi_arrival(j, k):
        return pltpu.make_async_remote_copy(
            src_ref=phi.at[:, cols(0)], dst_ref=block.at[k, rows(source(j)), :],
            send_sem=phi_ss.at[k, j], recv_sem=phi_rs.at[k, j],
            device_id={"band": peer(j)}, device_id_type=MESH)

    def back_copy(j, k):
        return pltpu.make_async_remote_copy(
            src_ref=mixed.at[k, rows(peer(j)), :], dst_ref=back.at[k, me],
            send_sem=back_ss.at[k, j], recv_sem=back_rs.at[k, j],
            device_id={"band": peer(j)}, device_id_type=MESH)

    def back_arrival(j, k):
        return pltpu.make_async_remote_copy(
            src_ref=mixed.at[k, rows(peer(j)), :], dst_ref=back.at[k, source(j)],
            send_sem=back_ss.at[k, j], recv_sem=back_rs.at[k, j],
            device_id={"band": peer(j)}, device_id_type=MESH)

    def terms_copy(j):
        return pltpu.make_async_remote_copy(
            src_ref=terms_send.at[rows(peer(j)), :], dst_ref=terms_recv.at[j],
            send_sem=terms_ss.at[j], recv_sem=terms_rs.at[j],
            device_id={"band": peer(j)}, device_id_type=MESH)

    def coef_copy(j):
        return pltpu.make_async_remote_copy(
            src_ref=coef_send, dst_ref=coef.at[rows(me), :],
            send_sem=coef_ss.at[j], recv_sem=coef_rs.at[j],
            device_id={"band": peer(j)}, device_id_type=MESH)

    def coef_arrival(j):
        return pltpu.make_async_remote_copy(
            src_ref=coef_send, dst_ref=coef.at[rows(source(j)), :],
            send_sem=coef_ss.at[j], recv_sem=coef_rs.at[j],
            device_id={"band": peer(j)}, device_id_type=MESH)

    def send_phi():
        def planes(k, carry):
            for j in range(PEERS - 1):
                phi_copy(j, k).start()
            return carry
        lax.fori_loop(0, DEPTH + 1, planes, 0)

    @pl.when(core == FIRST)
    def _():
        send_phi()

    def own_block(k, carry):
        plane = lax.rem(me * DEPTH + k, SIDE)
        block[k, rows(me), :] = phi[:, cols(plane)]
        return carry
    lax.fori_loop(0, DEPTH + 1, own_block, 0)

    def apply_plane(g, sums):
        norm, energy = sums
        fields = [phi[:, cols(g, c, LANES)].astype(jnp.float32) for c in range(SLICES)]
        ups, downs = upper(fields), lower(fields)
        after, before = lax.rem(g + 1, SIDE), lax.rem(g + SIDE - 1, SIDE)
        for c in range(SLICES):
            beside = ups[c] + downs[c]
            beside += phi[:, cols(after, c, LANES)].astype(jnp.float32)
            beside += phi[:, cols(before, c, LANES)].astype(jnp.float32)
            weight = pot[pl.ds(g * SLICES + c, 1), :] + 3.0
            image = (weight * fields[c] - 0.5 * beside).astype(jnp.bfloat16)
            applied[:, cols(g, c, LANES)] = image
            norm += fields[c] * fields[c]
            energy += fields[c] * image.astype(jnp.float32)
        return norm, energy
    zeros = jnp.zeros((OWN, LANES), jnp.float32)
    norm, energy = lax.fori_loop(0, SIDE, apply_plane, (zeros, zeros))
    norm = jnp.sum(norm, axis=1, keepdims=True)
    energy = jnp.sum(energy, axis=1, keepdims=True)

    @pl.when(core != FIRST)
    def _():
        pl.semaphore_wait(gate, 1)
        send_phi()

    def half_stencil(k, with_next):
        def some_rows(i, carry):
            r = rows(i)
            fields = [block[k, r, c * LANES:(c + 1) * LANES].astype(jnp.float32) for c in range(SLICES)]
            ups = upper(fields)
            for c in range(SLICES):
                beside = ups[c]
                if with_next:
                    beside += block[k + 1, r, c * LANES:(c + 1) * LANES].astype(jnp.float32)
                weight = 0.5 * pot[pl.ds((me * DEPTH + k) * SLICES + c, 1), :] + 1.5
                half[r, c * LANES:(c + 1) * LANES] = (weight * fields[c] - 0.5 * beside).astype(jnp.bfloat16)
            return carry
        lax.fori_loop(0, PEERS, some_rows, 0)

    for k in range(DEPTH):
        for j in range(PEERS - 1):
            phi_arrival(j, k).wait_recv()
        if k == GATE_AT:
            @pl.when(core == FIRST)
            def _():
                pl.semaphore_signal(gate, inc=1, device_id={"frag": partner}, device_id_type=MESH)
        if k == GATE_BACK_AT:
            @pl.when(core != FIRST)
            def _():
                pl.semaphore_signal(gate_back, inc=1, device_id={"frag": partner}, device_id_type=MESH)
        term = contract_rows(block[k], block[k])
        margin_sum[...] = term if k == 0 else margin_sum[...] + term
        if k >= 1:
            half_stencil(k - 1, True)
            term = contract_rows(block[k - 1], half[...])
            half_sum[...] = term if k == 1 else half_sum[...] + term
    half_stencil(DEPTH - 1, False)
    half_sum[...] += contract_rows(block[DEPTH - 1], half[...])
    for j in range(PEERS - 1):
        phi_arrival(j, DEPTH).wait_recv()
    total = half_sum[...] - 0.5 * contract_rows(block[DEPTH - 1], block[DEPTH])
    total = total + total.T
    column = lax.broadcasted_iota(jnp.int32, (BANDS, BANDS), 1)
    row = lax.broadcasted_iota(jnp.int32, (BANDS, BANDS), 0)
    above, below = column > row, column < row
    total = jnp.where(above, total, margin_sum[...])
    half_sum[...] = total
    terms_send[...] = total.astype(jnp.bfloat16)
    for j in range(PEERS - 1):
        terms_copy(j).start()
    own = half_sum[rows(me), :]
    for j in range(PEERS - 1):
        terms_copy(j).wait_recv()
        own += terms_recv[j].astype(jnp.float32)
    coef_send[...] = own.astype(jnp.bfloat16)
    for j in range(PEERS - 1):
        coef_copy(j).start()
    coef[rows(me), :] = own.astype(jnp.bfloat16)
    for j in range(PEERS - 1):
        coef_arrival(j).wait_recv()
    whole = coef[...].astype(jnp.float32)
    turned = whole.T
    half_sum[...] = turned
    for j in range(PEERS - 1):
        terms_copy(j).wait_send()
    terms_send[...] = jnp.where(above, whole, jnp.where(below, turned, 0.0)).astype(jnp.bfloat16)

    for k in range(DEPTH):
        mixed[k] = jnp.dot(terms_send[...], block[k], preferred_element_type=jnp.float32).astype(jnp.bfloat16)
        if k == 0:
            @pl.when(core == FIRST)
            def _():
                pl.semaphore_wait(gate_back, 1)
        for j in range(PEERS - 1):
            back_copy(j, k).start()

    own_column = lax.broadcasted_iota(jnp.int32, (OWN, BANDS), 1)
    own_row = lax.broadcasted_iota(jnp.int32, (OWN, BANDS), 0) + me * OWN
    own_turned = half_sum[rows(me), :]
    on_diagonal = own_column == own_row
    margin_ref[...] = jnp.where(on_diagonal, norm, jnp.where(own_column < own_row, own, own_turned))
    projected_ref[...] = jnp.where(on_diagonal, energy, jnp.where(own_column > own_row, own, own_turned))
    scale = 1.0 / norm
    own_coef = energy / norm

    def finish(k, b, taken):
        plane = b * DEPTH + k
        for c in range(SLICES):
            rest = applied[:, cols(plane, c, LANES)].astype(jnp.float32)
            rest -= own_coef * phi[:, cols(plane, c, LANES)].astype(jnp.float32)
            out_ref[:, cols(plane, c, LANES)] = (rest - scale * taken(c).astype(jnp.float32)).astype(jnp.bfloat16)

    def finish_own(k, carry):
        finish(k, me, lambda c: mixed[k, rows(me), c * LANES:(c + 1) * LANES])
        return carry
    lax.fori_loop(0, DEPTH, finish_own, 0)

    def finish_others(k, carry):
        for j in range(PEERS - 1):
            back_arrival(j, k).wait_recv()
            b = source(j)
            finish(k, b, lambda c: back[k, b, :, c * LANES:(c + 1) * LANES])
        return carry
    lax.fori_loop(0, DEPTH, finish_others, 0)

    for j in range(PEERS - 1):
        coef_copy(j).wait_send()

    def drain_phi(k, carry):
        for j in range(PEERS - 1):
            phi_copy(j, k).wait_send()
        return carry
    lax.fori_loop(0, DEPTH + 1, drain_phi, 0)

    def drain_back(k, carry):
        for j in range(PEERS - 1):
            back_copy(j, k).wait_send()
        return carry
    lax.fori_loop(0, DEPTH, drain_back, 0)


def put_out_kernel(res, margin, projected, res_out, margin_out, projected_out, sem):
    copies = [
        pltpu.make_async_copy(margin, margin_out, sem.at[4]),
        pltpu.make_async_copy(projected, projected_out, sem.at[5]),
    ]
    width = res.shape[1] // 4
    for i in range(4):
        part = pl.ds(i * width, width)
        copies.append(pltpu.make_async_copy(res.at[:, part], res_out.at[:, part], sem.at[i]))
    for copy in copies:
        copy.start()
    for copy in copies:
        copy.wait()


def put_out(*arrays):
    kept = [pltpu.with_memory_space_constraint(a, pltpu.VMEM) for a in arrays]
    return pl.pallas_call(
        put_out_kernel,
        out_shape=tuple(jax.ShapeDtypeStruct(a.shape, a.dtype) for a in arrays),
        in_specs=[pl.BlockSpec(memory_space=pltpu.VMEM)] * 3,
        out_specs=[pl.BlockSpec(memory_space=pl.ANY)] * 3,
        scratch_shapes=[pltpu.SemaphoreType.DMA((6,))],
        compiler_params=pltpu.CompilerParams(vmem_limit_bytes=8 << 20),
        name="put_out",
    )(*kept)


def shards(orbitals, potential):
    grid = orbitals.shape[1]
    bf16, f32 = jnp.bfloat16, jnp.float32
    dma = pltpu.SemaphoreType.DMA
    residuals, margin, projected = pl.pallas_call(
        kernel,
        out_shape=(
            pltpu.VMEM((OWN, grid), bf16),
            pltpu.VMEM((OWN, BANDS), f32),
            pltpu.VMEM((OWN, BANDS), f32),
        ),
        in_specs=[pl.BlockSpec(memory_space=pltpu.HBM)] * 2,
        out_specs=[pl.BlockSpec(memory_space=pltpu.VMEM)] * 3,
        scratch_shapes=[
            pltpu.VMEM((OWN, grid), bf16),
            pltpu.VMEM((grid // LANES, LANES), f32),
            pltpu.VMEM((OWN, grid), bf16),
            pltpu.VMEM((DEPTH + 1, BANDS, PLANE), bf16),
            pltpu.VMEM((BANDS, PLANE), bf16),
            pltpu.VMEM((BANDS, BANDS), f32),
            pltpu.VMEM((BANDS, BANDS), f32),
            pltpu.VMEM((BANDS, BANDS), bf16),
            pltpu.VMEM((PEERS - 1, OWN, BANDS), bf16),
            pltpu.VMEM((OWN, BANDS), bf16),
            pltpu.VMEM((BANDS, BANDS), bf16),
            pltpu.VMEM((DEPTH, BANDS, PLANE), bf16),
            pltpu.VMEM((DEPTH, PEERS, OWN, PLANE), bf16),
            dma((5,)),
            dma((DEPTH + 1, PEERS - 1)),
            dma((DEPTH + 1, PEERS - 1)),
            dma((PEERS - 1,)),
            dma((PEERS - 1,)),
            dma((PEERS - 1,)),
            dma((PEERS - 1,)),
            dma((DEPTH, PEERS - 1)),
            dma((DEPTH, PEERS - 1)),
            pltpu.SemaphoreType.REGULAR,
            pltpu.SemaphoreType.REGULAR,
        ],
        compiler_params=pltpu.CompilerParams(
            collective_id=0, has_side_effects=True, vmem_limit_bytes=40 << 20),
        name="subspace",
    )(
        pltpu.with_memory_space_constraint(orbitals, pltpu.HBM),
        pltpu.with_memory_space_constraint(potential.reshape(grid // LANES, LANES), pltpu.HBM),
    )
    residuals, margin, projected = put_out(residuals, margin, projected)
    return margin, projected, residuals


def solution(mesh):
    return jax.shard_map(
        shards,
        mesh=mesh,
        in_specs=(P(("frag", "band"), None), P("frag")),
        out_specs=(P(("frag", "band"), None), P(("frag", "band"), None), P(("frag", "band"), None)),
        check_vma=False,
    )
```

```python
import functools

import jax
import jax.numpy as jnp
from jax import lax
from jax.experimental import pallas as pl
from jax.experimental.pallas import tpu as pltpu
from jax.sharding import PartitionSpec as P

MESH = pl.DeviceIdType.MESH
SIDE = 32
PLANE = SIDE * SIDE
LANES = 128
SLICES = PLANE // LANES
OWN = 32
BANDS = 256
PEERS = 8
DEPTH = 4
HALF = PLANE // 2
QUADS = HALF // LANES
EDGE = HALF + 2 * LANES
OFFSETS = ((2, 1), (2, 0), (1, 1), (3, 1), (1, 0), (3, 0), (0, 1))
FIRST = 1
GATE_AT = 2
GATE_BACK_AT = 3


def contract_rows(left, right):
    return lax.dot_general(left, right, (((1,), (1,)), ((), ())), preferred_element_type=jnp.float32)


def kernel(
    phi_hbm, pot_hbm, out_ref, margin_ref, projected_ref,
    phi, pot, applied, block, half, edge_send, edge, last_rows, margin_sum, half_sum,
    terms_send, terms_recv, coef_send, coef, mixed, back,
    load_sem, phi_ss, phi_rs, edge_ss, edge_rs, terms_ss, terms_rs, coef_ss, coef_rs, back_ss, back_rs, gate, gate_back,
):
    me = lax.axis_index("band")
    frag = lax.axis_index("frag")
    core = lax.rem(frag, 2)
    x, z = me // 2, lax.rem(me, 2)
    partner = frag + 1 - 2 * core

    def peer(j):
        dx, dz = OFFSETS[j]
        return lax.rem(x + dx, 4) * 2 + lax.rem(z + dz, 2)

    def source(j):
        dx, dz = OFFSETS[j]
        return lax.rem(x + 4 - dx, 4) * 2 + lax.rem(z + dz, 2)

    def rows(b):
        return pl.ds(pl.multiple_of(b * OWN, OWN), OWN)

    def cols(plane, c=0, n=LANES):
        return pl.ds(pl.multiple_of(plane * PLANE + c * LANES, LANES), n)

    def half_cols(plane, c=0, n=LANES):
        return pl.ds(pl.multiple_of(plane * HALF + c * LANES, LANES), n)

    barrier = pltpu.get_barrier_semaphore()
    for j in range(PEERS - 1):
        pl.semaphore_signal(barrier, inc=1, device_id={"band": peer(j)}, device_id_type=MESH)
    pl.semaphore_signal(barrier, inc=1, device_id={"frag": partner}, device_id_type=MESH)
    pot_load = pltpu.make_async_copy(pot_hbm, pot, load_sem.at[2])
    pot_load.start()

    def load_plane(plane, carry):
        for h in range(2):
            pltpu.make_async_copy(
                phi_hbm.at[:, cols(plane, h * QUADS, HALF)], phi.at[h, :, half_cols(plane, 0, HALF)], load_sem.at[h],
            ).start()
        return carry
    lax.fori_loop(0, SIDE, load_plane, 0)
    for h in range(2):
        pltpu.make_async_copy(phi_hbm.at[:, 0:SIDE * HALF], phi.at[h], load_sem.at[h]).wait()
    pot_load.wait()
    pl.semaphore_wait(barrier, PEERS)

    lane = lax.broadcasted_iota(jnp.int32, (OWN, LANES), 1)
    z_pos = lax.rem(lane, SIDE)
    z_last, z_first = z_pos == SIDE - 1, z_pos == 0
    y_inner, y_outer = lane < LANES - SIDE, lane >= SIDE

    def upper(fields, beyond=None):
        ahead = [pltpu.roll(f, LANES - SIDE, 1) for f in fields]
        after = ahead[1:] + [ahead[0] if beyond is None else beyond]
        sums = []
        for c, f in enumerate(fields):
            y_up = jnp.where(y_inner, ahead[c], after[c])
            z_up = jnp.where(z_last, pltpu.roll(f, SIDE - 1, 1), pltpu.roll(f, LANES - 1, 1))
            sums.append(y_up + z_up)
        return sums

    def lower(fields):
        behind = [pltpu.roll(f, SIDE, 1) for f in fields]
        sums = []
        for c in range(SLICES):
            y_down = jnp.where(y_outer, behind[c], behind[(c - 1) % SLICES])
            z_down = jnp.where(z_first, pltpu.roll(fields[c], LANES - SIDE + 1, 1), pltpu.roll(fields[c], 1, 1))
            sums.append(y_down + z_down)
        return sums

    def phi_copy(j, k):
        p = peer(j)
        return pltpu.make_async_remote_copy(
            src_ref=phi.at[lax.rem(p, 2), :, half_cols(p // 2 * PEERS + 2 * k, 0, PLANE)],
            dst_ref=block.at[k, rows(me), :],
            send_sem=phi_ss.at[k, j], recv_sem=phi_rs.at[k, j],
            device_id={"band": p}, device_id_type=MESH)

    def phi_arrival(j, k):
        return pltpu.make_async_remote_copy(
            src_ref=phi.at[0, :, 0:PLANE], dst_ref=block.at[k, rows(source(j)), :],
            send_sem=phi_ss.at[k, j], recv_sem=phi_rs.at[k, j],
            device_id={"band": peer(j)}, device_id_type=MESH)

    def edge_copy(j):
        return pltpu.make_async_remote_copy(
            src_ref=edge_send.at[peer(j)], dst_ref=edge.at[rows(me), :],
            send_sem=edge_ss.at[j], recv_sem=edge_rs.at[j],
            device_id={"band": peer(j)}, device_id_type=MESH)

    def edge_arrival(j):
        return pltpu.make_async_remote_copy(
            src_ref=edge_send.at[peer(j)], dst_ref=edge.at[rows(source(j)), :],
            send_sem=edge_ss.at[j], recv_sem=edge_rs.at[j],
            device_id={"band": peer(j)}, device_id_type=MESH)

    def back_copy(j, k):
        return pltpu.make_async_remote_copy(
            src_ref=mixed.at[k, rows(peer(j)), :], dst_ref=back.at[k, me],
            send_sem=back_ss.at[k, j], recv_sem=back_rs.at[k, j],
            device_id={"band": peer(j)}, device_id_type=MESH)

    def back_arrival(j, k):
        return pltpu.make_async_remote_copy(
            src_ref=mixed.at[k, rows(peer(j)), :], dst_ref=back.at[k, source(j)],
            send_sem=back_ss.at[k, j], recv_sem=back_rs.at[k, j],
            device_id={"band": peer(j)}, device_id_type=MESH)

    def terms_copy(j):
        return pltpu.make_async_remote_copy(
            src_ref=terms_send.at[rows(peer(j)), :], dst_ref=terms_recv.at[j],
            send_sem=terms_ss.at[j], recv_sem=terms_rs.at[j],
            device_id={"band": peer(j)}, device_id_type=MESH)

    def coef_copy(j):
        return pltpu.make_async_remote_copy(
            src_ref=coef_send, dst_ref=coef.at[rows(me), :],
            send_sem=coef_ss.at[j], recv_sem=coef_rs.at[j],
            device_id={"band": peer(j)}, device_id_type=MESH)

    def coef_arrival(j):
        return pltpu.make_async_remote_copy(
            src_ref=coef_send, dst_ref=coef.at[rows(source(j)), :],
            send_sem=coef_ss.at[j], recv_sem=coef_rs.at[j],
            device_id={"band": peer(j)}, device_id_type=MESH)

    def send_phi():
        def chunks(k, carry):
            for j in range(PEERS - 1):
                phi_copy(j, k).start()
            return carry
        lax.fori_loop(0, DEPTH, chunks, 0)

    def send_edges():
        for j in range(PEERS - 1):
            edge_copy(j).start()

    @pl.when(core == FIRST)
    def _():
        send_phi()

    strip = lane // SIDE

    def packed(fields, at):
        rolled = [pltpu.roll(f, (i * SIDE - at) % LANES, 1) if i * SIDE != at else f for i, f in enumerate(fields)]
        return jnp.where(strip < 2, jnp.where(strip == 0, rolled[0], rolled[1]), jnp.where(strip == 2, rolled[2], rolled[3]))

    def fill_edge(p, carry):
        px, pz = p // 2, lax.rem(p, 2)
        edge_send[p, :, 0:HALF] = phi[pz, :, half_cols(lax.rem(px * PEERS + PEERS, SIDE), 0, HALF)]
        for m in range(2):
            fields = [phi[1 - pz, :, half_cols(px * PEERS + 4 * m + i)].astype(jnp.float32) for i in range(4)]
            edge_send[p, :, HALF + m * LANES:HALF + (m + 1) * LANES] = packed(fields, 0).astype(jnp.bfloat16)
        return carry
    lax.fori_loop(0, PEERS, fill_edge, 0)

    @pl.when(core == FIRST)
    def _():
        send_edges()

    def own_block(k, carry):
        block[k, rows(me), :] = phi[z, :, half_cols(x * PEERS + 2 * k, 0, PLANE)]
        return carry
    lax.fori_loop(0, DEPTH, own_block, 0)
    edge[rows(me), :] = edge_send[me]

    def apply_plane(g, sums):
        norm, energy = sums
        def slices(plane):
            return [phi[c // QUADS, :, half_cols(plane, c % QUADS)].astype(jnp.float32) for c in range(SLICES)]
        fields = slices(g)
        ups, downs = upper(fields), lower(fields)
        after, before = slices(lax.rem(g + 1, SIDE)), slices(lax.rem(g + SIDE - 1, SIDE))
        for c in range(SLICES):
            beside = ups[c] + downs[c] + after[c] + before[c]
            weight = pot[pl.ds(g * SLICES + c, 1), :] + 3.0
            image = (weight * fields[c] - 0.5 * beside).astype(jnp.bfloat16)
            applied[:, cols(g, c)] = image
            norm += fields[c] * fields[c]
            energy += fields[c] * image.astype(jnp.float32)
        return norm, energy
    zeros = jnp.zeros((OWN, LANES), jnp.float32)
    norm, energy = lax.fori_loop(0, SIDE, apply_plane, (zeros, zeros))
    norm = jnp.sum(norm, axis=1, keepdims=True)
    energy = jnp.sum(energy, axis=1, keepdims=True)

    @pl.when(core != FIRST)
    def _():
        pl.semaphore_wait(gate, 1)
        send_phi()
        send_edges()

    def part(c):
        return slice(c * LANES, (c + 1) * LANES)

    def half_stencil(k, with_next):
        def some_rows(i, carry):
            r = rows(i)
            fields = [block[k, r, part(c)].astype(jnp.float32) for c in range(SLICES)]
            nothing = jnp.zeros((OWN, LANES), jnp.float32)
            ups = upper(fields[:QUADS], nothing) + upper(fields[QUADS:], nothing)
            for c in range(SLICES):
                beside = ups[c]
                if c < QUADS:
                    beside += fields[c + QUADS]
                elif with_next:
                    beside += block[k + 1, r, part(c - QUADS)].astype(jnp.float32)
                plane = x * PEERS + 2 * k + c // QUADS
                weight = 0.5 * pot[pl.ds(plane * SLICES + z * QUADS + c % QUADS, 1), :] + 1.5
                half[r, part(c)] = (weight * fields[c] - 0.5 * beside).astype(jnp.bfloat16)
            return carry
        lax.fori_loop(0, PEERS, some_rows, 0)

    def fill_last_rows(i, carry):
        r = rows(i)
        for m in range(2):
            fields = [
                block[2 * m + s // 2, r, part(s % 2 * QUADS + QUADS - 1)].astype(jnp.float32) for s in range(4)
            ]
            last_rows[r, part(m)] = packed(fields, LANES - SIDE).astype(jnp.bfloat16)
        return carry

    for k in range(DEPTH):
        for j in range(PEERS - 1):
            phi_arrival(j, k).wait_recv()
        if k == GATE_AT:
            @pl.when(core == FIRST)
            def _():
                pl.semaphore_signal(gate, inc=1, device_id={"frag": partner}, device_id_type=MESH)
        if k == GATE_BACK_AT:
            @pl.when(core != FIRST)
            def _():
                pl.semaphore_signal(gate_back, inc=1, device_id={"frag": partner}, device_id_type=MESH)
        term = contract_rows(block[k], block[k])
        margin_sum[...] = term if k == 0 else margin_sum[...] + term
        if k >= 1:
            half_stencil(k - 1, True)
            term = contract_rows(block[k - 1], half[...])
            half_sum[...] = term if k == 1 else half_sum[...] + term
    half_stencil(DEPTH - 1, False)
    total = half_sum[...] + contract_rows(block[DEPTH - 1], half[...])
    half_sum[...] = total + total.T
    lax.fori_loop(0, PEERS, fill_last_rows, 0)
    for j in range(PEERS - 1):
        edge_arrival(j).wait_recv()
    inner = (block[DEPTH - 1, :, HALF:PLANE], last_rows[...])
    outer = (edge[:, 0:HALF], edge[:, HALF:EDGE])
    across = sum(contract_rows(a, b) + contract_rows(b, a) for a, b in zip(inner, outer))
    total = half_sum[...] - 0.5 * across
    column = lax.broadcasted_iota(jnp.int32, (BANDS, BANDS), 1)
    row = lax.broadcasted_iota(jnp.int32, (BANDS, BANDS), 0)
    above, below = column > row, column < row
    total = jnp.where(above, total, margin_sum[...])
    half_sum[...] = total
    terms_send[...] = total.astype(jnp.bfloat16)
    for j in range(PEERS - 1):
        terms_copy(j).start()
    own = half_sum[rows(me), :]
    for j in range(PEERS - 1):
        terms_copy(j).wait_recv()
        own += terms_recv[j].astype(jnp.float32)
    coef_send[...] = own.astype(jnp.bfloat16)
    for j in range(PEERS - 1):
        coef_copy(j).start()
    coef[rows(me), :] = own.astype(jnp.bfloat16)
    for j in range(PEERS - 1):
        coef_arrival(j).wait_recv()
    whole = coef[...].astype(jnp.float32)
    turned = whole.T
    half_sum[...] = turned
    for j in range(PEERS - 1):
        terms_copy(j).wait_send()
    terms_send[...] = jnp.where(above, whole, jnp.where(below, turned, 0.0)).astype(jnp.bfloat16)

    for k in range(DEPTH):
        mixed[k] = jnp.dot(terms_send[...], block[k], preferred_element_type=jnp.float32).astype(jnp.bfloat16)
        if k == 0:
            @pl.when(core == FIRST)
            def _():
                pl.semaphore_wait(gate_back, 1)
        for j in range(PEERS - 1):
            back_copy(j, k).start()

    own_column = lax.broadcasted_iota(jnp.int32, (OWN, BANDS), 1)
    own_row = lax.broadcasted_iota(jnp.int32, (OWN, BANDS), 0) + me * OWN
    own_turned = half_sum[rows(me), :]
    on_diagonal = own_column == own_row
    margin_ref[...] = jnp.where(on_diagonal, norm, jnp.where(own_column < own_row, own, own_turned))
    projected_ref[...] = jnp.where(on_diagonal, energy, jnp.where(own_column > own_row, own, own_turned))
    scale = 1.0 / norm
    own_coef = energy / norm

    def finish(k, b, taken):
        bx, bz = b // 2, lax.rem(b, 2)
        for c in range(SLICES):
            plane = bx * PEERS + 2 * k + c // QUADS
            place = cols(plane, bz * QUADS + c % QUADS)
            rest = applied[:, place].astype(jnp.float32)
            rest -= own_coef * phi[bz, :, half_cols(plane, c % QUADS)].astype(jnp.float32)
            out_ref[:, place] = (rest - scale * taken(c).astype(jnp.float32)).astype(jnp.bfloat16)

    def finish_own(k, carry):
        finish(k, me, lambda c: mixed[k, rows(me), c * LANES:(c + 1) * LANES])
        return carry
    lax.fori_loop(0, DEPTH, finish_own, 0)

    def finish_others(k, carry):
        for j in range(PEERS - 1):
            back_arrival(j, k).wait_recv()
            b = source(j)
            finish(k, b, lambda c: back[k, b, :, c * LANES:(c + 1) * LANES])
        return carry
    lax.fori_loop(0, DEPTH, finish_others, 0)

    for j in range(PEERS - 1):
        coef_copy(j).wait_send()
        edge_copy(j).wait_send()

    def drain_phi(k, carry):
        for j in range(PEERS - 1):
            phi_copy(j, k).wait_send()
        return carry
    lax.fori_loop(0, DEPTH, drain_phi, 0)

    def drain_back(k, carry):
        for j in range(PEERS - 1):
            back_copy(j, k).wait_send()
        return carry
    lax.fori_loop(0, DEPTH, drain_back, 0)


def put_out_kernel(res, margin, projected, res_out, margin_out, projected_out, sem):
    copies = [
        pltpu.make_async_copy(margin, margin_out, sem.at[4]),
        pltpu.make_async_copy(projected, projected_out, sem.at[5]),
    ]
    width = res.shape[1] // 4
    for i in range(4):
        part = pl.ds(i * width, width)
        copies.append(pltpu.make_async_copy(res.at[:, part], res_out.at[:, part], sem.at[i]))
    for copy in copies:
        copy.start()
    for copy in copies:
        copy.wait()


def put_out(*arrays):
    kept = [pltpu.with_memory_space_constraint(a, pltpu.VMEM) for a in arrays]
    return pl.pallas_call(
        put_out_kernel,
        out_shape=tuple(jax.ShapeDtypeStruct(a.shape, a.dtype) for a in arrays),
        in_specs=[pl.BlockSpec(memory_space=pltpu.VMEM)] * 3,
        out_specs=[pl.BlockSpec(memory_space=pl.ANY)] * 3,
        scratch_shapes=[pltpu.SemaphoreType.DMA((6,))],
        compiler_params=pltpu.CompilerParams(vmem_limit_bytes=8 << 20),
        name="put_out",
    )(*kept)


def shards(orbitals, potential):
    grid = orbitals.shape[1]
    bf16, f32 = jnp.bfloat16, jnp.float32
    dma = pltpu.SemaphoreType.DMA
    residuals, margin, projected = pl.pallas_call(
        kernel,
        out_shape=(
            pltpu.VMEM((OWN, grid), bf16),
            pltpu.VMEM((OWN, BANDS), f32),
            pltpu.VMEM((OWN, BANDS), f32),
        ),
        in_specs=[pl.BlockSpec(memory_space=pltpu.HBM)] * 2,
        out_specs=[pl.BlockSpec(memory_space=pltpu.VMEM)] * 3,
        scratch_shapes=[
            pltpu.VMEM((2, OWN, grid // 2), bf16),
            pltpu.VMEM((grid // LANES, LANES), f32),
            pltpu.VMEM((OWN, grid), bf16),
            pltpu.VMEM((DEPTH, BANDS, PLANE), bf16),
            pltpu.VMEM((BANDS, PLANE), bf16),
            pltpu.VMEM((PEERS, OWN, EDGE), bf16),
            pltpu.VMEM((BANDS, EDGE), bf16),
            pltpu.VMEM((BANDS, 2 * LANES), bf16),
            pltpu.VMEM((BANDS, BANDS), f32),
            pltpu.VMEM((BANDS, BANDS), f32),
            pltpu.VMEM((BANDS, BANDS), bf16),
            pltpu.VMEM((PEERS - 1, OWN, BANDS), bf16),
            pltpu.VMEM((OWN, BANDS), bf16),
            pltpu.VMEM((BANDS, BANDS), bf16),
            pltpu.VMEM((DEPTH, BANDS, PLANE), bf16),
            pltpu.VMEM((DEPTH, PEERS, OWN, PLANE), bf16),
            dma((3,)),
            dma((DEPTH, PEERS - 1)),
            dma((DEPTH, PEERS - 1)),
            dma((PEERS - 1,)),
            dma((PEERS - 1,)),
            dma((PEERS - 1,)),
            dma((PEERS - 1,)),
            dma((PEERS - 1,)),
            dma((PEERS - 1,)),
            dma((DEPTH, PEERS - 1)),
            dma((DEPTH, PEERS - 1)),
            pltpu.SemaphoreType.REGULAR,
            pltpu.SemaphoreType.REGULAR,
        ],
        compiler_params=pltpu.CompilerParams(
            collective_id=0, has_side_effects=True, vmem_limit_bytes=40 << 20),
        name="subspace",
    )(
        pltpu.with_memory_space_constraint(orbitals, pltpu.HBM),
        pltpu.with_memory_space_constraint(potential.reshape(grid // LANES, LANES), pltpu.HBM),
    )
    residuals, margin, projected = put_out(residuals, margin, projected)
    return margin, projected, residuals


def solution(mesh):
    return jax.shard_map(
        shards,
        mesh=mesh,
        in_specs=(P(("frag", "band"), None), P("frag")),
        out_specs=(P(("frag", "band"), None), P(("frag", "band"), None), P(("frag", "band"), None)),
        check_vma=False,
    )
```

```python
import functools

import jax
import jax.numpy as jnp
from jax import lax
from jax.experimental import pallas as pl
from jax.experimental.pallas import tpu as pltpu
from jax.sharding import PartitionSpec as P

MESH = pl.DeviceIdType.MESH
SIDE = 32
PLANE = SIDE * SIDE
LANES = 128
SLICES = PLANE // LANES
OWN = 32
BANDS = 256
PEERS = 8
DEPTH = 4
HALF = PLANE // 2
QUADS = HALF // LANES
EDGE = HALF + 2 * LANES
OFFSETS = ((2, 1), (2, 0), (1, 1), (3, 1), (1, 0), (3, 0), (0, 1))
FIRST = 1
GATE_AT = 2
GATE_BACK_AT = 3


def contract_rows(left, right):
    return lax.dot_general(left, right, (((1,), (1,)), ((), ())), preferred_element_type=jnp.float32)


def kernel(
    phi_hbm, pot_hbm, out_ref, margin_ref, projected_ref,
    phi, pot, applied, sums, table, block, half, edge_send, edge, last_rows, margin_sum, half_sum,
    terms_send, terms_recv, coef_send, coef, mixed, back,
    load_sem, send_sem, recv_sem, phi_rs, back_rs, last_rs, gate, gate_back,
):
    me = lax.axis_index("band")
    frag = lax.axis_index("frag")
    core = lax.rem(frag, 2)
    x, z = me // 2, lax.rem(me, 2)
    partner = frag + 1 - 2 * core

    def peer(j):
        dx, dz = OFFSETS[j]
        return lax.rem(x + dx, 4) * 2 + lax.rem(z + dz, 2)

    def source(j):
        dx, dz = OFFSETS[j]
        return lax.rem(x + 4 - dx, 4) * 2 + lax.rem(z + dz, 2)

    def rows(b):
        return pl.ds(pl.multiple_of(b * OWN, OWN), OWN)

    def cols(plane, c=0, n=LANES):
        return pl.ds(pl.multiple_of(plane * PLANE + c * LANES, LANES), n)

    def half_cols(plane, c=0, n=LANES):
        return pl.ds(pl.multiple_of(plane * HALF + c * LANES, LANES), n)

    barrier = pltpu.get_barrier_semaphore()
    for j in range(PEERS - 1):
        pl.semaphore_signal(barrier, inc=1, device_id={"band": peer(j)}, device_id_type=MESH)
    pl.semaphore_signal(barrier, inc=1, device_id={"frag": partner}, device_id_type=MESH)
    pot_load = pltpu.make_async_copy(pot_hbm, pot, load_sem.at[2])
    pot_load.start()

    def load_plane(plane, carry):
        for h in range(2):
            pltpu.make_async_copy(
                phi_hbm.at[:, cols(plane, h * QUADS, HALF)], phi.at[h, :, half_cols(plane, 0, HALF)], load_sem.at[h],
            ).start()
        return carry
    lax.fori_loop(0, SIDE, load_plane, 0)
    for h in range(2):
        pltpu.make_async_copy(phi_hbm.at[:, 0:SIDE * HALF], phi.at[h], load_sem.at[h]).wait()
    pot_load.wait()
    pl.semaphore_wait(barrier, PEERS)

    lane = lax.broadcasted_iota(jnp.int32, (OWN, LANES), 1)
    z_pos = lax.rem(lane, SIDE)
    z_last, z_first = z_pos == SIDE - 1, z_pos == 0
    y_inner, y_outer = lane < LANES - SIDE, lane >= SIDE

    def upper(fields, beyond=None):
        ahead = [pltpu.roll(f, LANES - SIDE, 1) for f in fields]
        after = ahead[1:] + [ahead[0] if beyond is None else beyond]
        sums = []
        for c, f in enumerate(fields):
            y_up = jnp.where(y_inner, ahead[c], after[c])
            z_up = jnp.where(z_last, pltpu.roll(f, SIDE - 1, 1), pltpu.roll(f, LANES - 1, 1))
            sums.append(y_up + z_up)
        return sums

    def lower(fields):
        behind = [pltpu.roll(f, SIDE, 1) for f in fields]
        sums = []
        for c in range(SLICES):
            y_down = jnp.where(y_outer, behind[c], behind[(c - 1) % SLICES])
            z_down = jnp.where(z_first, pltpu.roll(fields[c], LANES - SIDE + 1, 1), pltpu.roll(fields[c], 1, 1))
            sums.append(y_down + z_down)
        return sums

    def phi_copy(j, k):
        p = peer(j)
        return pltpu.make_async_remote_copy(
            src_ref=phi.at[lax.rem(p, 2), :, half_cols(p // 2 * PEERS + 2 * k, 0, PLANE)],
            dst_ref=block.at[k, rows(me), :],
            send_sem=send_sem.at[0], recv_sem=phi_rs.at[k],
            device_id={"band": p}, device_id_type=MESH)

    def edge_copy(j):
        return pltpu.make_async_remote_copy(
            src_ref=edge_send.at[peer(j)], dst_ref=edge.at[rows(me), :],
            send_sem=send_sem.at[1], recv_sem=recv_sem.at[1],
            device_id={"band": peer(j)}, device_id_type=MESH)

    def back_copy(j, k):
        return pltpu.make_async_remote_copy(
            src_ref=mixed.at[k, rows(peer(j)), :], dst_ref=back.at[k, me],
            send_sem=send_sem.at[4], recv_sem=last_rs.at[j] if k == DEPTH - 1 else back_rs.at[k],
            device_id={"band": peer(j)}, device_id_type=MESH)

    def all_sent(ref, i):
        pltpu.make_async_remote_copy(
            src_ref=ref, dst_ref=ref, send_sem=send_sem.at[i], recv_sem=recv_sem.at[0],
            device_id={"band": peer(0)}, device_id_type=MESH).wait_send()

    def all_received(ref, semaphore):
        pltpu.make_async_remote_copy(
            src_ref=ref, dst_ref=ref, send_sem=send_sem.at[0], recv_sem=semaphore,
            device_id={"band": peer(0)}, device_id_type=MESH).wait_recv()

    others = pl.ds(0, BANDS - OWN)

    def terms_copy(j):
        return pltpu.make_async_remote_copy(
            src_ref=terms_send.at[rows(peer(j)), :], dst_ref=terms_recv.at[j],
            send_sem=send_sem.at[2], recv_sem=recv_sem.at[2],
            device_id={"band": peer(j)}, device_id_type=MESH)

    def coef_copy(j):
        return pltpu.make_async_remote_copy(
            src_ref=coef_send, dst_ref=coef.at[rows(me), :],
            send_sem=send_sem.at[3], recv_sem=recv_sem.at[3],
            device_id={"band": peer(j)}, device_id_type=MESH)

    def send_phi():
        def chunks(k, carry):
            for j in range(PEERS - 1):
                phi_copy(j, k).start()
            return carry
        lax.fori_loop(0, DEPTH, chunks, 0)

    def send_edges():
        for j in range(PEERS - 1):
            edge_copy(j).start()

    @pl.when(core == FIRST)
    def _():
        send_phi()

    strip = lane // SIDE

    def packed(fields, at):
        rolled = [pltpu.roll(f, (i * SIDE - at) % LANES, 1) if i * SIDE != at else f for i, f in enumerate(fields)]
        return jnp.where(strip < 2, jnp.where(strip == 0, rolled[0], rolled[1]), jnp.where(strip == 2, rolled[2], rolled[3]))

    def fill_edge(p, carry):
        px, pz = p // 2, lax.rem(p, 2)
        edge_send[p, :, 0:HALF] = phi[pz, :, half_cols(lax.rem(px * PEERS + PEERS, SIDE), 0, HALF)]
        for m in range(2):
            fields = [phi[1 - pz, :, half_cols(px * PEERS + 4 * m + i)].astype(jnp.float32) for i in range(4)]
            edge_send[p, :, HALF + m * LANES:HALF + (m + 1) * LANES] = packed(fields, 0).astype(jnp.bfloat16)
        return carry
    lax.fori_loop(0, PEERS, fill_edge, 0)

    @pl.when(core == FIRST)
    def _():
        send_edges()

    def own_block(k, carry):
        block[k, rows(me), :] = phi[z, :, half_cols(x * PEERS + 2 * k, 0, PLANE)]
        return carry
    lax.fori_loop(0, DEPTH, own_block, 0)
    edge[rows(me), :] = edge_send[me]

    def apply_plane(g, carry):
        norm, energy = carry
        def slices(plane):
            return [phi[c // QUADS, :, half_cols(plane, c % QUADS)].astype(jnp.float32) for c in range(SLICES)]
        fields = slices(g)
        ups, downs = upper(fields), lower(fields)
        after, before = slices(lax.rem(g + 1, SIDE)), slices(lax.rem(g + SIDE - 1, SIDE))
        for c in range(SLICES):
            beside = ups[c] + downs[c] + after[c] + before[c]
            weight = pot[pl.ds(g * SLICES + c, 1), :] + 3.0
            image = (weight * fields[c] - 0.5 * beside).astype(jnp.bfloat16)
            applied[:, cols(g, c)] = image
            norm += fields[c] * fields[c]
            energy += fields[c] * image.astype(jnp.float32)
        return norm, energy

    def apply_planes(first, last):
        zeros = jnp.zeros((OWN, LANES), jnp.float32)
        norm, energy = lax.fori_loop(first, last, apply_plane, (zeros, zeros))
        sums[0] = norm if first == 0 else sums[0] + norm
        sums[1] = energy if first == 0 else sums[1] + energy

    def fill_table(i, carry):
        there = lax.broadcasted_iota(jnp.int32, (SIDE, HALF), 0)
        here = lax.broadcasted_iota(jnp.int32, (SIDE, HALF), 1)
        here_y, here_z = here // SIDE, lax.rem(here, SIDE)
        same_y, same_z = here_y == i, there == here_z
        up_z = same_y & (there == lax.rem(here_z + 1, SIDE))
        up_y = (here_y == i - 1) & same_z
        values = jnp.where(same_y & same_z, 1.5, 0.0) - jnp.where(up_z | up_y, 0.5, 0.0)
        table[rows(i), :] = values.astype(jnp.bfloat16)
        return carry
    lax.fori_loop(0, HALF // SIDE, fill_table, 0)

    @pl.when(core != FIRST)
    def _():
        apply_planes(0, SIDE)
        pl.semaphore_wait(gate, 1)
        send_phi()
        send_edges()

    def part(c):
        return slice(c * LANES, (c + 1) * LANES)

    def half_stencil(k):
        for u in range(2):
            plane = x * PEERS + 2 * k + u
            inside = jnp.dot(block[k, :, u * HALF:(u + 1) * HALF], table[...], preferred_element_type=jnp.float32)
            for c in range(QUADS):
                here = part(u * QUADS + c)
                weight = 0.5 * pot[pl.ds(plane * SLICES + z * QUADS + c, 1), :]
                value = inside[:, part(c)] + weight * block[k, :, here].astype(jnp.float32)
                if u == 0:
                    value -= 0.5 * block[k, :, part(QUADS + c)].astype(jnp.float32)
                half[:, here] = value.astype(jnp.bfloat16)

    def fill_last_rows(m):
        def some_rows(i, carry):
            r = rows(i)
            fields = [
                block[2 * m + s // 2, r, part(s % 2 * QUADS + QUADS - 1)].astype(jnp.float32) for s in range(4)
            ]
            last_rows[r, part(m)] = packed(fields, LANES - SIDE).astype(jnp.bfloat16)
            return carry
        lax.fori_loop(0, PEERS, some_rows, 0)

    for k in range(DEPTH):
        all_received(block.at[k, others, :], phi_rs.at[k])
        if k == GATE_AT:
            @pl.when(core == FIRST)
            def _():
                pl.semaphore_signal(gate, inc=1, device_id={"frag": partner}, device_id_type=MESH)
        if k == GATE_BACK_AT:
            @pl.when(core != FIRST)
            def _():
                pl.semaphore_signal(gate_back, inc=1, device_id={"frag": partner}, device_id_type=MESH)
        term = contract_rows(block[k], block[k])
        margin_sum[...] = term if k == 0 else margin_sum[...] + term
        half_stencil(k)
        term = contract_rows(block[k], half[...])
        if k >= 1:
            term -= 0.5 * contract_rows(block[k - 1, :, HALF:PLANE], block[k, :, 0:HALF])
        half_sum[...] = term if k == 0 else half_sum[...] + term
        if k % 2 == 1:
            fill_last_rows(k // 2)
    half_sum[...] = half_sum[...] + half_sum[...].T
    all_received(edge.at[others, :], recv_sem.at[1])
    inner = (block[DEPTH - 1, :, HALF:PLANE], last_rows[...])
    outer = (edge[:, 0:HALF], edge[:, HALF:EDGE])
    across = sum(contract_rows(a, b) + contract_rows(b, a) for a, b in zip(inner, outer))
    total = half_sum[...] - 0.5 * across
    column = lax.broadcasted_iota(jnp.int32, (BANDS, BANDS), 1)
    row = lax.broadcasted_iota(jnp.int32, (BANDS, BANDS), 0)
    above, below = column > row, column < row
    total = jnp.where(above, total, margin_sum[...])
    half_sum[...] = total
    terms_send[...] = total.astype(jnp.bfloat16)
    for j in range(PEERS - 1):
        terms_copy(j).start()

    @pl.when(core == FIRST)
    def _():
        apply_planes(0, SIDE // 2)

    own = half_sum[rows(me), :]
    all_received(terms_recv, recv_sem.at[2])
    for j in range(PEERS - 1):
        own += terms_recv[j].astype(jnp.float32)
    coef_send[...] = own.astype(jnp.bfloat16)
    for j in range(PEERS - 1):
        coef_copy(j).start()
    coef[rows(me), :] = own.astype(jnp.bfloat16)

    @pl.when(core == FIRST)
    def _():
        apply_planes(SIDE // 2, SIDE)

    all_received(coef.at[others, :], recv_sem.at[3])
    whole = coef[...].astype(jnp.float32)
    turned = whole.T
    half_sum[...] = turned
    all_sent(terms_send.at[others, :], 2)
    terms_send[...] = jnp.where(above, whole, jnp.where(below, turned, 0.0)).astype(jnp.bfloat16)

    for k in range(DEPTH):
        mixed[k] = jnp.dot(terms_send[...], block[k], preferred_element_type=jnp.float32).astype(jnp.bfloat16)
        if k == 0:
            @pl.when(core == FIRST)
            def _():
                pl.semaphore_wait(gate_back, 1)
        for j in range(PEERS - 1):
            back_copy(j, k).start()

    norm = jnp.sum(sums[0], axis=1, keepdims=True)
    energy = jnp.sum(sums[1], axis=1, keepdims=True)
    own_column = lax.broadcasted_iota(jnp.int32, (OWN, BANDS), 1)
    own_row = lax.broadcasted_iota(jnp.int32, (OWN, BANDS), 0) + me * OWN
    own_turned = half_sum[rows(me), :]
    on_diagonal = own_column == own_row
    margin_ref[...] = jnp.where(on_diagonal, norm, jnp.where(own_column < own_row, own, own_turned))
    projected_ref[...] = jnp.where(on_diagonal, energy, jnp.where(own_column > own_row, own, own_turned))
    scale = 1.0 / norm
    own_coef = energy / norm

    def finish(k, b, taken):
        bx, bz = b // 2, lax.rem(b, 2)
        for c in range(SLICES):
            plane = bx * PEERS + 2 * k + c // QUADS
            place = cols(plane, bz * QUADS + c % QUADS)
            rest = applied[:, place].astype(jnp.float32)
            rest -= own_coef * phi[bz, :, half_cols(plane, c % QUADS)].astype(jnp.float32)
            out_ref[:, place] = (rest - scale * taken(c).astype(jnp.float32)).astype(jnp.bfloat16)

    def finish_own(k, carry):
        finish(k, me, lambda c: mixed[k, rows(me), c * LANES:(c + 1) * LANES])
        return carry
    lax.fori_loop(0, DEPTH, finish_own, 0)

    def finish_from(k, j):
        b = source(j)
        finish(k, b, lambda c: back[k, b, :, c * LANES:(c + 1) * LANES])

    def finish_others(k, carry):
        all_received(back.at[k, pl.ds(0, PEERS - 1)], back_rs.at[k])
        for j in range(PEERS - 1):
            finish_from(k, j)
        return carry
    lax.fori_loop(0, DEPTH - 1, finish_others, 0)
    for j in range(PEERS - 1):
        all_received(back.at[DEPTH - 1, source(j)], last_rs.at[j])
        finish_from(DEPTH - 1, j)

    all_sent(block.at[:, others, :], 0)
    all_sent(edge.at[others, :], 1)
    all_sent(coef.at[others, :], 3)
    all_sent(mixed.at[:, others, :], 4)


def put_out_kernel(res, margin, projected, res_out, margin_out, projected_out, sem):
    copies = [
        pltpu.make_async_copy(margin, margin_out, sem.at[4]),
        pltpu.make_async_copy(projected, projected_out, sem.at[5]),
    ]
    width = res.shape[1] // 4
    for i in range(4):
        part = pl.ds(i * width, width)
        copies.append(pltpu.make_async_copy(res.at[:, part], res_out.at[:, part], sem.at[i]))
    for copy in copies:
        copy.start()
    for copy in copies:
        copy.wait()


def put_out(*arrays):
    kept = [pltpu.with_memory_space_constraint(a, pltpu.VMEM) for a in arrays]
    return pl.pallas_call(
        put_out_kernel,
        out_shape=tuple(jax.ShapeDtypeStruct(a.shape, a.dtype) for a in arrays),
        in_specs=[pl.BlockSpec(memory_space=pltpu.VMEM)] * 3,
        out_specs=[pl.BlockSpec(memory_space=pl.ANY)] * 3,
        scratch_shapes=[pltpu.SemaphoreType.DMA((6,))],
        compiler_params=pltpu.CompilerParams(vmem_limit_bytes=8 << 20),
        name="put_out",
    )(*kept)


def shards(orbitals, potential):
    grid = orbitals.shape[1]
    bf16, f32 = jnp.bfloat16, jnp.float32
    dma = pltpu.SemaphoreType.DMA
    residuals, margin, projected = pl.pallas_call(
        kernel,
        out_shape=(
            pltpu.VMEM((OWN, grid), bf16),
            pltpu.VMEM((OWN, BANDS), f32),
            pltpu.VMEM((OWN, BANDS), f32),
        ),
        in_specs=[pl.BlockSpec(memory_space=pltpu.HBM)] * 2,
        out_specs=[pl.BlockSpec(memory_space=pltpu.VMEM)] * 3,
        scratch_shapes=[
            pltpu.VMEM((2, OWN, grid // 2), bf16),
            pltpu.VMEM((grid // LANES, LANES), f32),
            pltpu.VMEM((OWN, grid), bf16),
            pltpu.VMEM((2, OWN, LANES), f32),
            pltpu.VMEM((HALF, HALF), bf16),
            pltpu.VMEM((DEPTH, BANDS, PLANE), bf16),
            pltpu.VMEM((BANDS, PLANE), bf16),
            pltpu.VMEM((PEERS, OWN, EDGE), bf16),
            pltpu.VMEM((BANDS, EDGE), bf16),
            pltpu.VMEM((BANDS, 2 * LANES), bf16),
            pltpu.VMEM((BANDS, BANDS), f32),
            pltpu.VMEM((BANDS, BANDS), f32),
            pltpu.VMEM((BANDS, BANDS), bf16),
            pltpu.VMEM((PEERS - 1, OWN, BANDS), bf16),
            pltpu.VMEM((OWN, BANDS), bf16),
            pltpu.VMEM((BANDS, BANDS), bf16),
            pltpu.VMEM((DEPTH, BANDS, PLANE), bf16),
            pltpu.VMEM((DEPTH, PEERS, OWN, PLANE), bf16),
            dma((3,)),
            dma((5,)),
            dma((4,)),
            dma((DEPTH,)),
            dma((DEPTH - 1,)),
            dma((PEERS - 1,)),
            pltpu.SemaphoreType.REGULAR,
            pltpu.SemaphoreType.REGULAR,
        ],
        compiler_params=pltpu.CompilerParams(
            collective_id=0, has_side_effects=True, vmem_limit_bytes=40 << 20),
        name="subspace",
    )(
        pltpu.with_memory_space_constraint(orbitals, pltpu.HBM),
        pltpu.with_memory_space_constraint(potential.reshape(grid // LANES, LANES), pltpu.HBM),
    )
    residuals, margin, projected = put_out(residuals, margin, projected)
    return margin, projected, residuals


def solution(mesh):
    return jax.shard_map(
        shards,
        mesh=mesh,
        in_specs=(P(("frag", "band"), None), P("frag")),
        out_specs=(P(("frag", "band"), None), P(("frag", "band"), None), P(("frag", "band"), None)),
        check_vma=False,
    )
```

```python
import functools

import jax
import jax.numpy as jnp
from jax import lax
from jax.experimental import pallas as pl
from jax.experimental.pallas import tpu as pltpu
from jax.sharding import PartitionSpec as P

MESH = pl.DeviceIdType.MESH
SIDE = 32
PLANE = SIDE * SIDE
LANES = 128
SLICES = PLANE // LANES
OWN = 32
BANDS = 256
PEERS = 8
DEPTH = 4
HALF = PLANE // 2
QUADS = HALF // LANES
EDGE = HALF + 2 * LANES
OFFSETS = ((2, 1), (2, 0), (1, 1), (3, 1), (1, 0), (3, 0), (0, 1))
FIRST = 1
GATE_AT = 2
GATE_BACK_AT = 3


def contract_rows(left, right):
    return lax.dot_general(left, right, (((1,), (1,)), ((), ())), preferred_element_type=jnp.float32)


def kernel(
    phi_hbm, pot_hbm, out_ref, margin_ref, projected_ref,
    phi, pot, applied, sums, table, block, half, edge_send, edge, surface, margin_sum, half_sum,
    terms_send, terms_recv, coef_send, coef, mixed, back,
    load_sem, send_sem, recv_sem, phi_rs, back_rs, last_rs, gate, gate_back,
):
    me = lax.axis_index("band")
    frag = lax.axis_index("frag")
    core = lax.rem(frag, 2)
    x, z = me // 2, lax.rem(me, 2)
    partner = frag + 1 - 2 * core

    def peer(j):
        dx, dz = OFFSETS[j]
        return lax.rem(x + dx, 4) * 2 + lax.rem(z + dz, 2)

    def source(j):
        dx, dz = OFFSETS[j]
        return lax.rem(x + 4 - dx, 4) * 2 + lax.rem(z + dz, 2)

    def rows(b):
        return pl.ds(pl.multiple_of(b * OWN, OWN), OWN)

    def cols(plane, c=0, n=LANES):
        return pl.ds(pl.multiple_of(plane * PLANE + c * LANES, LANES), n)

    def half_cols(plane, c=0, n=LANES):
        return pl.ds(pl.multiple_of(plane * HALF + c * LANES, LANES), n)

    barrier = pltpu.get_barrier_semaphore()
    for j in range(PEERS - 1):
        pl.semaphore_signal(barrier, inc=1, device_id={"band": peer(j)}, device_id_type=MESH)
    pl.semaphore_signal(barrier, inc=1, device_id={"frag": partner}, device_id_type=MESH)
    pot_load = pltpu.make_async_copy(pot_hbm, pot, load_sem.at[2])
    pot_load.start()

    def load_plane(plane, carry):
        for h in range(2):
            pltpu.make_async_copy(
                phi_hbm.at[:, cols(plane, h * QUADS, HALF)], phi.at[h, :, half_cols(plane, 0, HALF)], load_sem.at[h],
            ).start()
        return carry
    lax.fori_loop(0, SIDE, load_plane, 0)
    for h in range(2):
        pltpu.make_async_copy(phi_hbm.at[:, 0:SIDE * HALF], phi.at[h], load_sem.at[h]).wait()
    pot_load.wait()
    pl.semaphore_wait(barrier, PEERS)

    lane = lax.broadcasted_iota(jnp.int32, (OWN, LANES), 1)
    z_pos = lax.rem(lane, SIDE)
    z_last, z_first = z_pos == SIDE - 1, z_pos == 0
    y_inner, y_outer = lane < LANES - SIDE, lane >= SIDE

    def upper(fields, beyond=None):
        ahead = [pltpu.roll(f, LANES - SIDE, 1) for f in fields]
        after = ahead[1:] + [ahead[0] if beyond is None else beyond]
        sums = []
        for c, f in enumerate(fields):
            y_up = jnp.where(y_inner, ahead[c], after[c])
            z_up = jnp.where(z_last, pltpu.roll(f, SIDE - 1, 1), pltpu.roll(f, LANES - 1, 1))
            sums.append(y_up + z_up)
        return sums

    def lower(fields):
        behind = [pltpu.roll(f, SIDE, 1) for f in fields]
        sums = []
        for c in range(SLICES):
            y_down = jnp.where(y_outer, behind[c], behind[(c - 1) % SLICES])
            z_down = jnp.where(z_first, pltpu.roll(fields[c], LANES - SIDE + 1, 1), pltpu.roll(fields[c], 1, 1))
            sums.append(y_down + z_down)
        return sums

    def phi_copy(j, k):
        p = peer(j)
        return pltpu.make_async_remote_copy(
            src_ref=phi.at[lax.rem(p, 2), :, half_cols(p // 2 * PEERS + 2 * k, 0, PLANE)],
            dst_ref=block.at[k, rows(me), :],
            send_sem=send_sem.at[0], recv_sem=phi_rs.at[k],
            device_id={"band": p}, device_id_type=MESH)

    def edge_copy(j):
        return pltpu.make_async_remote_copy(
            src_ref=edge_send.at[peer(j)], dst_ref=edge.at[rows(me), :],
            send_sem=send_sem.at[1], recv_sem=recv_sem.at[1],
            device_id={"band": peer(j)}, device_id_type=MESH)

    def back_copy(j, k, here):
        return pltpu.make_async_remote_copy(
            src_ref=mixed.at[k, rows(peer(j)), here], dst_ref=back.at[k, me, :, here],
            send_sem=send_sem.at[4], recv_sem=last_rs.at[j] if k == DEPTH - 1 else back_rs.at[k],
            device_id={"band": peer(j)}, device_id_type=MESH)

    def all_sent(ref, i):
        pltpu.make_async_remote_copy(
            src_ref=ref, dst_ref=ref, send_sem=send_sem.at[i], recv_sem=recv_sem.at[0],
            device_id={"band": peer(0)}, device_id_type=MESH).wait_send()

    def all_received(ref, semaphore):
        pltpu.make_async_remote_copy(
            src_ref=ref, dst_ref=ref, send_sem=send_sem.at[0], recv_sem=semaphore,
            device_id={"band": peer(0)}, device_id_type=MESH).wait_recv()

    others = pl.ds(0, BANDS - OWN)

    def terms_copy(j):
        return pltpu.make_async_remote_copy(
            src_ref=terms_send.at[rows(peer(j)), :], dst_ref=terms_recv.at[j],
            send_sem=send_sem.at[2], recv_sem=recv_sem.at[2],
            device_id={"band": peer(j)}, device_id_type=MESH)

    def coef_copy(j):
        return pltpu.make_async_remote_copy(
            src_ref=coef_send, dst_ref=coef.at[rows(me), :],
            send_sem=send_sem.at[3], recv_sem=recv_sem.at[3],
            device_id={"band": peer(j)}, device_id_type=MESH)

    def send_phi():
        def chunks(k, carry):
            for j in range(PEERS - 1):
                phi_copy(j, k).start()
            return carry
        lax.fori_loop(0, DEPTH, chunks, 0)

    def send_edges():
        for j in range(PEERS - 1):
            edge_copy(j).start()

    @pl.when(core == FIRST)
    def _():
        send_phi()

    strip = lane // SIDE

    def packed(fields, at):
        rolled = [pltpu.roll(f, (i * SIDE - at) % LANES, 1) if i * SIDE != at else f for i, f in enumerate(fields)]
        return jnp.where(strip < 2, jnp.where(strip == 0, rolled[0], rolled[1]), jnp.where(strip == 2, rolled[2], rolled[3]))

    def fill_edge(p, carry):
        px, pz = p // 2, lax.rem(p, 2)
        edge_send[p, :, 0:HALF] = phi[pz, :, half_cols(lax.rem(px * PEERS + PEERS, SIDE), 0, HALF)]
        for m in range(2):
            fields = [phi[1 - pz, :, half_cols(px * PEERS + 4 * m + i)].astype(jnp.float32) for i in range(4)]
            edge_send[p, :, HALF + m * LANES:HALF + (m + 1) * LANES] = packed(fields, 0).astype(jnp.bfloat16)
        return carry
    lax.fori_loop(0, PEERS, fill_edge, 0)

    @pl.when(core == FIRST)
    def _():
        send_edges()

    def own_block(k, carry):
        block[k, rows(me), :] = phi[z, :, half_cols(x * PEERS + 2 * k, 0, PLANE)]
        return carry
    lax.fori_loop(0, DEPTH, own_block, 0)
    edge[rows(me), :] = edge_send[me]

    def apply_plane(g, carry):
        norm, energy = carry
        def slices(plane):
            return [phi[c // QUADS, :, half_cols(plane, c % QUADS)].astype(jnp.float32) for c in range(SLICES)]
        fields = slices(g)
        ups, downs = upper(fields), lower(fields)
        after, before = slices(lax.rem(g + 1, SIDE)), slices(lax.rem(g + SIDE - 1, SIDE))
        for c in range(SLICES):
            beside = ups[c] + downs[c] + after[c] + before[c]
            weight = pot[pl.ds(g * SLICES + c, 1), :] + 3.0
            image = (weight * fields[c] - 0.5 * beside).astype(jnp.bfloat16)
            applied[:, cols(g, c)] = image
            norm += fields[c] * fields[c]
            energy += fields[c] * image.astype(jnp.float32)
        return norm, energy

    def apply_planes(first, last):
        zeros = jnp.zeros((OWN, LANES), jnp.float32)
        norm, energy = lax.fori_loop(first, last, apply_plane, (zeros, zeros))
        sums[0] = norm if first == 0 else sums[0] + norm
        sums[1] = energy if first == 0 else sums[1] + energy

    def fill_table(i, carry):
        there = lax.broadcasted_iota(jnp.int32, (SIDE, HALF), 0)
        here = lax.broadcasted_iota(jnp.int32, (SIDE, HALF), 1)
        here_y, here_z = here // SIDE, lax.rem(here, SIDE)
        same_y, same_z = here_y == i, there == here_z
        up_z = same_y & (there == lax.rem(here_z + 1, SIDE))
        up_y = (here_y == i - 1) & same_z
        values = jnp.where(same_y & same_z, 1.5, 0.0) - jnp.where(up_z | up_y, 0.5, 0.0)
        table[rows(i), :] = values.astype(jnp.bfloat16)
        return carry
    lax.fori_loop(0, HALF // SIDE, fill_table, 0)

    @pl.when(core != FIRST)
    def _():
        apply_planes(0, SIDE)
        pl.semaphore_wait(gate, 1)
        send_phi()
        send_edges()

    def part(c):
        return slice(c * LANES, (c + 1) * LANES)

    def half_stencil(k):
        for u in range(2):
            plane = x * PEERS + 2 * k + u
            inside = jnp.dot(block[k, :, u * HALF:(u + 1) * HALF], table[...], preferred_element_type=jnp.float32)
            for c in range(QUADS):
                here = part(u * QUADS + c)
                weight = 0.5 * pot[pl.ds(plane * SLICES + z * QUADS + c, 1), :]
                value = inside[:, part(c)] + weight * block[k, :, here].astype(jnp.float32)
                if u == 0:
                    value -= 0.5 * block[k, :, part(QUADS + c)].astype(jnp.float32)
                half[:, here] = value.astype(jnp.bfloat16)

    def fill_last_rows(m):
        def some_rows(i, carry):
            r = rows(i)
            fields = [
                block[2 * m + s // 2, r, part(s % 2 * QUADS + QUADS - 1)].astype(jnp.float32) for s in range(4)
            ]
            surface[r, part(QUADS + m)] = packed(fields, LANES - SIDE).astype(jnp.bfloat16)
            return carry
        lax.fori_loop(0, PEERS, some_rows, 0)

    for k in range(DEPTH):
        all_received(block.at[k, others, :], phi_rs.at[k])
        if k == GATE_AT:
            @pl.when(core == FIRST)
            def _():
                pl.semaphore_signal(gate, inc=1, device_id={"frag": partner}, device_id_type=MESH)
        if k == GATE_BACK_AT:
            @pl.when(core != FIRST)
            def _():
                pl.semaphore_signal(gate_back, inc=1, device_id={"frag": partner}, device_id_type=MESH)
        term = contract_rows(block[k], block[k])
        margin_sum[...] = term if k == 0 else margin_sum[...] + term
        half_stencil(k)
        term = contract_rows(block[k], half[...])
        if k >= 1:
            term -= 0.5 * contract_rows(block[k - 1, :, HALF:PLANE], block[k, :, 0:HALF])
        half_sum[...] = term if k == 0 else half_sum[...] + term
        if k % 2 == 1:
            fill_last_rows(k // 2)
    half_sum[...] = half_sum[...] + half_sum[...].T
    surface[:, 0:HALF] = block[DEPTH - 1, :, HALF:PLANE]
    all_received(edge.at[others, :], recv_sem.at[1])
    across = contract_rows(surface[...], edge[...]) + contract_rows(edge[...], surface[...])
    total = half_sum[...] - 0.5 * across
    column = lax.broadcasted_iota(jnp.int32, (BANDS, BANDS), 1)
    row = lax.broadcasted_iota(jnp.int32, (BANDS, BANDS), 0)
    above, below = column > row, column < row
    total = jnp.where(above, total, margin_sum[...])
    half_sum[...] = total
    terms_send[...] = total.astype(jnp.bfloat16)
    for j in range(PEERS - 1):
        terms_copy(j).start()

    @pl.when(core == FIRST)
    def _():
        apply_planes(0, SIDE // 2)

    own = half_sum[rows(me), :]
    all_received(terms_recv, recv_sem.at[2])
    for j in range(PEERS - 1):
        own += terms_recv[j].astype(jnp.float32)
    coef_send[...] = own.astype(jnp.bfloat16)
    for j in range(PEERS - 1):
        coef_copy(j).start()
    coef[rows(me), :] = own.astype(jnp.bfloat16)

    @pl.when(core == FIRST)
    def _():
        apply_planes(SIDE // 2, SIDE)

    all_received(coef.at[others, :], recv_sem.at[3])
    whole = coef[...].astype(jnp.float32)
    turned = whole.T
    half_sum[...] = turned
    all_sent(terms_send.at[others, :], 2)
    terms_send[...] = jnp.where(above, whole, jnp.where(below, turned, 0.0)).astype(jnp.bfloat16)

    for k, here in [(0, pl.ds(0, HALF)), (0, pl.ds(HALF, HALF))] + [(k, pl.ds(0, PLANE)) for k in range(1, DEPTH)]:
        mixed[k, :, here] = jnp.dot(
            terms_send[...], block[k, :, here], preferred_element_type=jnp.float32).astype(jnp.bfloat16)
        if (k, here.start) == (0, 0):
            @pl.when(core == FIRST)
            def _():
                pl.semaphore_wait(gate_back, 1)
        for j in range(PEERS - 1):
            back_copy(j, k, here).start()

    norm = jnp.sum(sums[0], axis=1, keepdims=True)
    energy = jnp.sum(sums[1], axis=1, keepdims=True)
    own_column = lax.broadcasted_iota(jnp.int32, (OWN, BANDS), 1)
    own_row = lax.broadcasted_iota(jnp.int32, (OWN, BANDS), 0) + me * OWN
    own_turned = half_sum[rows(me), :]
    on_diagonal = own_column == own_row
    margin_ref[...] = jnp.where(on_diagonal, norm, jnp.where(own_column < own_row, own, own_turned))
    projected_ref[...] = jnp.where(on_diagonal, energy, jnp.where(own_column > own_row, own, own_turned))
    scale = 1.0 / norm
    own_coef = energy / norm

    def finish(k, b, taken):
        bx, bz = b // 2, lax.rem(b, 2)
        for c in range(SLICES):
            plane = bx * PEERS + 2 * k + c // QUADS
            place = cols(plane, bz * QUADS + c % QUADS)
            rest = applied[:, place].astype(jnp.float32)
            rest -= own_coef * phi[bz, :, half_cols(plane, c % QUADS)].astype(jnp.float32)
            out_ref[:, place] = (rest - scale * taken(c).astype(jnp.float32)).astype(jnp.bfloat16)

    def finish_own(k, carry):
        finish(k, me, lambda c: mixed[k, rows(me), c * LANES:(c + 1) * LANES])
        return carry
    lax.fori_loop(0, DEPTH, finish_own, 0)

    def finish_from(k, j):
        b = source(j)
        finish(k, b, lambda c: back[k, b, :, c * LANES:(c + 1) * LANES])

    def finish_others(k, carry):
        all_received(back.at[k, pl.ds(0, PEERS - 1)], back_rs.at[k])
        for j in range(PEERS - 1):
            finish_from(k, j)
        return carry
    lax.fori_loop(0, DEPTH - 1, finish_others, 0)
    for j in range(PEERS - 1):
        all_received(back.at[DEPTH - 1, source(j)], last_rs.at[j])
        finish_from(DEPTH - 1, j)

    all_sent(block.at[:, others, :], 0)
    all_sent(edge.at[others, :], 1)
    all_sent(coef.at[others, :], 3)
    all_sent(mixed.at[:, others, :], 4)


def put_out_kernel(res, margin, projected, res_out, margin_out, projected_out, sem):
    width = res.shape[1] // 4
    for i in range(4):
        part = pl.ds(i * width, width)
        pltpu.make_async_copy(res.at[:, part], res_out.at[:, part], sem.at[0]).start()
    small = [
        pltpu.make_async_copy(margin, margin_out, sem.at[1]),
        pltpu.make_async_copy(projected, projected_out, sem.at[2]),
    ]
    for copy in small:
        copy.start()
    for copy in small:
        copy.wait()
    pltpu.make_async_copy(res, res_out, sem.at[0]).wait()


def put_out(*arrays):
    kept = [pltpu.with_memory_space_constraint(a, pltpu.VMEM) for a in arrays]
    return pl.pallas_call(
        put_out_kernel,
        out_shape=tuple(jax.ShapeDtypeStruct(a.shape, a.dtype) for a in arrays),
        in_specs=[pl.BlockSpec(memory_space=pltpu.VMEM)] * 3,
        out_specs=[pl.BlockSpec(memory_space=pl.ANY)] * 3,
        scratch_shapes=[pltpu.SemaphoreType.DMA((3,))],
        compiler_params=pltpu.CompilerParams(vmem_limit_bytes=8 << 20),
        name="put_out",
    )(*kept)


def shards(orbitals, potential):
    grid = orbitals.shape[1]
    bf16, f32 = jnp.bfloat16, jnp.float32
    dma = pltpu.SemaphoreType.DMA
    residuals, margin, projected = pl.pallas_call(
        kernel,
        out_shape=(
            pltpu.VMEM((OWN, grid), bf16),
            pltpu.VMEM((OWN, BANDS), f32),
            pltpu.VMEM((OWN, BANDS), f32),
        ),
        in_specs=[pl.BlockSpec(memory_space=pltpu.HBM)] * 2,
        out_specs=[pl.BlockSpec(memory_space=pltpu.VMEM)] * 3,
        scratch_shapes=[
            pltpu.VMEM((2, OWN, grid // 2), bf16),
            pltpu.VMEM((grid // LANES, LANES), f32),
            pltpu.VMEM((OWN, grid), bf16),
            pltpu.VMEM((2, OWN, LANES), f32),
            pltpu.VMEM((HALF, HALF), bf16),
            pltpu.VMEM((DEPTH, BANDS, PLANE), bf16),
            pltpu.VMEM((BANDS, PLANE), bf16),
            pltpu.VMEM((PEERS, OWN, EDGE), bf16),
            pltpu.VMEM((BANDS, EDGE), bf16),
            pltpu.VMEM((BANDS, EDGE), bf16),
            pltpu.VMEM((BANDS, BANDS), f32),
            pltpu.VMEM((BANDS, BANDS), f32),
            pltpu.VMEM((BANDS, BANDS), bf16),
            pltpu.VMEM((PEERS - 1, OWN, BANDS), bf16),
            pltpu.VMEM((OWN, BANDS), bf16),
            pltpu.VMEM((BANDS, BANDS), bf16),
            pltpu.VMEM((DEPTH, BANDS, PLANE), bf16),
            pltpu.VMEM((DEPTH, PEERS, OWN, PLANE), bf16),
            dma((3,)),
            dma((5,)),
            dma((4,)),
            dma((DEPTH,)),
            dma((DEPTH - 1,)),
            dma((PEERS - 1,)),
            pltpu.SemaphoreType.REGULAR,
            pltpu.SemaphoreType.REGULAR,
        ],
        compiler_params=pltpu.CompilerParams(
            collective_id=0, has_side_effects=True, vmem_limit_bytes=40 << 20),
        name="subspace",
    )(
        pltpu.with_memory_space_constraint(orbitals, pltpu.HBM),
        pltpu.with_memory_space_constraint(potential.reshape(grid // LANES, LANES), pltpu.HBM),
    )
    residuals, margin, projected = put_out(residuals, margin, projected)
    return margin, projected, residuals


def solution(mesh):
    return jax.shard_map(
        shards,
        mesh=mesh,
        in_specs=(P(("frag", "band"), None), P("frag")),
        out_specs=(P(("frag", "band"), None), P(("frag", "band"), None), P(("frag", "band"), None)),
        check_vma=False,
    )
```
